32 devices in a mesh: dp: 4 (over y, x), seq: 8 (over z, core).
Axes of the slice: x: 2, y: 2, z: 4, core: 2. Of those that a mesh axis runs over, the one named last changes fastest.
Arguments:
- stream: bfloat16 [4, 256, 1536], P('dp', 'seq'), may hold values from -6 to 6
- queries: bfloat16 [4, 256, 1536], P('dp', 'seq'), may hold values from -30 to 30
- new_keys: bfloat16 [4, 256, 1536], P('dp', 'seq'), may hold values from -6.5 to 6.5
- new_values: bfloat16 [4, 256, 1536], P('dp', 'seq'), may hold values from -6 to 6
- cache_keys: bfloat16 [4, 768, 1536], P('dp', 'seq'), may hold values from -6.375 to 6.375
- cache_values: bfloat16 [4, 768, 1536], P('dp', 'seq'), may hold values from -6 to 6
- cache_frames: int32 [4, 768], P('dp', 'seq'), may hold values from 0 to 20, as said below
- group_index: int32 [4], P('dp'), may hold values from 4 to 7, as said below
- timestep: int32 [4], P('dp'), may hold values from 0 to 3
- gate_table: float32 [4, 1536], replicated, may hold values from 0.1 to 1.9
- attn_out_weight: bfloat16 [1536, 1536], replicated, may hold values from -0.15625 to 0.15625
- critic_in: bfloat16 [32768, 1536], P(('dp', 'seq')), may hold values from -6 to 6
- critic_cot: bfloat16 [32768, 1536], P(('dp', 'seq')), may hold values from -6 to 6
- critic_weight: bfloat16 [1536, 1536], P(('dp', 'seq')), may hold values from -0.15625 to 0.15625
Outputs:
- stream_out: bfloat16 [4, 256, 1536], P('dp', 'seq')
- critic_grad_in: bfloat16 [32768, 1536], P(('dp', 'seq'))
- critic_grad_weight: float32 [1536, 1536], P(('dp', 'seq'))
The draws below stay inside these ranges and needn't reach their ends.
Inputs may be any that keep to these rules, and one draw needn't show every extreme that they name: `group_index`: index of the frame group; both ends are reached in every draw. `cache_frames`: sample b's cache holds the 12 frames 3 * group_index[b] - 12 to 3 * group_index[b] - 1, each in one contiguous run of slots, runs of equal length up to one slot, in a rotated order.
All inputs are finite; a program needn't handle non-finite values.
Results may differ from the reference program's by a relative error of at most 0.0045.
Values may be sent and summed in bfloat16 or wider, within the bound.
A program may use at most 128 MiB of HBM per device.

```python
import jax
import jax.numpy as jnp
from jax import lax

D = 1536
HEADS = 12
HEAD = 128
STEPS = 4
FRAMES_GROUP = 3
WINDOW_FRAMES = 9
BATCH = 4
GROUP = 256
CACHE = 768
CRIT_ROWS = 32768


def drawn_pair(key):
    base = jax.random.fold_in(key, 4711)
    key_q, key_k = jax.random.split(base, 2)
    query_draw = jnp.clip(1.6 * jax.random.normal(key_q, (BATCH, GROUP, D), jnp.float32), -6.4, 6.4)
    key_draw = jnp.clip(1.6 * jax.random.normal(key_k, (BATCH, GROUP, D), jnp.float32), -6.4, 6.4)
    return (query_draw, key_draw)


def draw_queries(key, part):
    return drawn_pair(key)[0].astype(jnp.bfloat16)


def draw_new_keys(key, part):
    return drawn_pair(key)[1].astype(jnp.bfloat16)


def frame_layout(key):
    base = jax.random.fold_in(key, 9173)
    key_group, key_turn = jax.random.split(base, 2)
    cycle = FRAMES_GROUP + WINDOW_FRAMES
    group = jax.random.randint(key_group, (BATCH,), 4, 8, dtype=jnp.int32)
    group = group.at[0].set(7).at[BATCH - 1].set(4)
    turn = jax.random.randint(key_turn, (BATCH, 1), 0, cycle, dtype=jnp.int32)
    block = jnp.arange(CACHE, dtype=jnp.int32) * cycle // CACHE
    frames = FRAMES_GROUP * group[:, None] - cycle + (block[None, :] + turn) % cycle
    return (group, frames.astype(jnp.int32))


def draw_group_index(key, part):
    return frame_layout(key)[0]


def draw_cache_frames(key, part):
    return frame_layout(key)[1]


def plant(drawn, own_key, low, top_value):
    longest = drawn.shape.index(max(drawn.shape))
    spots = []
    for shift in (0, 1):
        where = [jax.random.randint(jax.random.fold_in(own_key, axis), (), 0, length) for axis, length in enumerate(drawn.shape)]
        where[longest] = (where[longest] + shift) % drawn.shape[longest]
        spots.append(tuple(where))
    return drawn.at[spots[0]].set(low).at[spots[1]].set(top_value)


def strengthened(entries, stream_key, source, target, parts, factor):
    def block_of(axis_at):
        return (jnp.arange(entries.shape[axis_at]) // (entries.shape[axis_at] // parts)).reshape((-1,) + (1,) * (entries.ndim - 1 - axis_at))

    one_side = jax.random.permutation(stream_key, parts)[block_of(target)]
    other_side = (block_of(target) + parts // 2) % parts
    return jnp.where((block_of(source) == one_side) | (block_of(source) == other_side), factor * entries, entries)


def shard_levels(key, shape, cuts, least, largest):
    def one(position, shards_of):
        heights = jax.random.uniform(jax.random.fold_in(jax.random.fold_in(key, 6), position), (shards_of,), jnp.float32, least / len(cuts), largest / len(cuts))
        return jnp.repeat(jnp.exp(heights), shape[position] // shards_of).reshape((-1,) + (1,) * (len(shape) - position - 1))

    loudness = one(*cuts[0])
    for cut in cuts[1:]:
        loudness = loudness * one(*cut)
    return loudness


def noise(key, shape, spread, limit, cuts=(), held_as=jnp.bfloat16):
    factor_of = shard_levels(key, shape, cuts, -0.22, 0.18) if cuts else 1.0
    values = jax.random.normal(key, shape, jnp.float32) * spread * factor_of
    return jnp.minimum(jnp.maximum(values, -limit), limit).astype(held_as)


def noise_with(key, shape, scale, bound, cuts, heavy, kind=jnp.bfloat16):
    array = scale * jax.random.normal(key, shape, jnp.float32)
    if cuts:
        array = array * shard_levels(key, shape, cuts, -0.22, 0.18)
    return jnp.clip(strengthened(array, jax.random.fold_in(key, 3), *heavy), -bound, bound).astype(kind)


def setup_inputs(seed: int = 0) -> dict:
    key_list = jax.random.split(jax.random.key(seed), 15)
    stream = noise(key_list[0], (BATCH, GROUP, D), 1.0, 6.0, ((0, 4), (1, 8)))
    queries = draw_queries(jax.random.fold_in(key_list[14], 71), 0)
    new_keys = draw_new_keys(jax.random.fold_in(key_list[14], 71), 0)
    new_values = noise(key_list[3], (BATCH, GROUP, D), 1.0, 6.0, ((0, 4), (1, 8)))
    cache_keys = noise(key_list[4], (BATCH, CACHE, D), 1.6, 6.375, ((0, 4), (1, 8)))
    cache_values = noise(key_list[5], (BATCH, CACHE, D), 1.0, 6.0, ((0, 4), (1, 8)))
    cache_frames = draw_cache_frames(jax.random.fold_in(key_list[14], 71), 0)
    group_index = draw_group_index(jax.random.fold_in(key_list[14], 71), 0)
    timestep = plant(jax.random.randint(key_list[8], (BATCH,), 0, STEPS), jax.random.fold_in(key_list[8], 1), 0, STEPS - 1).astype(jnp.int32)
    gate_table = jnp.clip(1.0 + 0.18 * jax.random.normal(key_list[9], (STEPS, D), jnp.float32), 0.1, 1.9)
    attn_out_weight = noise(key_list[10], (D, D), D ** -0.5, 0.15625)
    critic_in = noise_with(key_list[11], (CRIT_ROWS, D), 1.0, 6.0, ((0, 32),), (0, 1, 32, 2.75))
    critic_cot = noise(key_list[12], (CRIT_ROWS, D), 1.0, 6.0, ((0, 32),))
    critic_weight = noise(key_list[13], (D, D), D ** -0.5, 0.15625, ((0, 32),))
    return {"stream": stream, "queries": queries, "new_keys": new_keys, "new_values": new_values, "cache_keys": cache_keys, "cache_values": cache_values, "cache_frames": cache_frames, "group_index": group_index, "timestep": timestep, "gate_table": gate_table, "attn_out_weight": attn_out_weight, "critic_in": critic_in, "critic_cot": critic_cot, "critic_weight": critic_weight}


def attend_sample(packed):
    query_block, key_new, value_new, key_cache, value_cache, frames, group = packed
    keys = jnp.concatenate([key_cache, key_new], axis=0)
    values = jnp.concatenate([value_cache, value_new], axis=0)
    first = FRAMES_GROUP * group
    live_cache = (frames < first) & (frames >= first - WINDOW_FRAMES)
    live = jnp.concatenate([live_cache, jnp.ones((GROUP,), dtype=bool)])
    query_heads = query_block.reshape(GROUP, HEADS, HEAD).transpose(1, 0, 2)
    key_heads = keys.reshape(GROUP + CACHE, HEADS, HEAD).transpose(1, 0, 2)
    value_heads = values.reshape(GROUP + CACHE, HEADS, HEAD).transpose(1, 0, 2)

    def one_head(triple):
        q_head, k_head, v_head = triple
        scores = jnp.dot(q_head, k_head.T, preferred_element_type=jnp.float32) * (HEAD ** -0.5)
        scores = jnp.where(live[None, :], scores, -1e30)
        top = jnp.max(scores, axis=1, keepdims=True)
        weights = jnp.where(live[None, :], jnp.exp(scores - top), 0.0)
        totals = jnp.sum(weights, axis=1, keepdims=True)
        summed = jnp.dot(weights.astype(jnp.bfloat16), v_head, preferred_element_type=jnp.float32)
        return summed / totals

    mixed = lax.map(one_head, (query_heads, key_heads, value_heads))
    return mixed.transpose(1, 0, 2).reshape(GROUP, D).astype(jnp.bfloat16)


def reference(stream, queries, new_keys, new_values, cache_keys, cache_values, cache_frames, group_index, timestep, gate_table, attn_out_weight, critic_in, critic_cot, critic_weight):
    mixed = lax.map(attend_sample, (queries, new_keys, new_values, cache_keys, cache_values, cache_frames, group_index))
    projected = jnp.dot(mixed.reshape(BATCH * GROUP, D), attn_out_weight, preferred_element_type=jnp.float32).reshape(BATCH, GROUP, D)
    onehot = (timestep[:, None] == jnp.arange(STEPS, dtype=jnp.int32)[None, :]).astype(jnp.float32)
    gate = jnp.dot(onehot, gate_table, precision=lax.Precision.HIGHEST)
    stream_out = (stream.astype(jnp.float32) + gate[:, None, :] * projected).astype(jnp.bfloat16)
    grad_in = jnp.dot(critic_cot, critic_weight.T, preferred_element_type=jnp.float32).astype(jnp.bfloat16)
    grad_weight = jnp.dot(critic_in.T, critic_cot, preferred_element_type=jnp.float32) * (float(CRIT_ROWS) ** -0.5)
    return (stream_out, grad_in, grad_weight)
```

```python
import functools

import jax
import jax.numpy as jnp
from jax import lax
from jax.experimental import pallas as pl
from jax.experimental.pallas import tpu as pltpu
from jax.sharding import PartitionSpec as P

HEADS = 12
HEAD = 128
FRAMES_GROUP = 3
WINDOW_FRAMES = 9
VMEM_LIMIT = 44 * 1024 * 1024
FINISH_LIMIT = 8 * 1024 * 1024


def critic_pass(critic_in, critic_cot, critic_weight):
    grad_in = lax.dot_general(
        critic_cot,
        lax.all_gather(critic_weight, ("dp", "seq"), axis=0, tiled=True),
        (((1,), (1,)), ((), ())),
        preferred_element_type=jnp.float32,
    ).astype(jnp.bfloat16)
    factor = float(critic_in.shape[0] * lax.axis_size(("dp", "seq"))) ** (-0.5)
    whole_term = (
        lax.dot_general(
            critic_in, critic_cot, (((0,), (0,)), ((), ())), preferred_element_type=jnp.float32
        )
        * factor
    )
    grad_weight = lax.psum_scatter(whole_term, ("dp", "seq"), scatter_dimension=0, tiled=True)
    return (grad_in, grad_weight)


def by_collectives(
    stream,
    queries,
    new_keys,
    new_values,
    cache_keys,
    cache_values,
    cache_frames,
    group_index,
    timestep,
    gate_table,
    attn_out_weight,
    critic_in,
    critic_cot,
    critic_weight,
):
    query_local = queries[0]
    own_rows = query_local.shape[0]
    width = query_local.shape[1]
    scale = HEAD ** (-0.5)
    first_frame = FRAMES_GROUP * group_index[0]
    frames = cache_frames[0]
    live_cache = (frames < first_frame) & (frames >= first_frame - WINDOW_FRAMES)
    live_local = jnp.concatenate([live_cache, jnp.ones((own_rows,), dtype=bool)])
    keys_local = jnp.concatenate([cache_keys[0], new_keys[0]], axis=0)
    values_local = jnp.concatenate([cache_values[0], new_values[0]], axis=0)
    all_queries = lax.all_gather(queries, "seq", axis=1, tiled=True)[0]
    total_rows = all_queries.shape[0]
    query_heads = all_queries.reshape(total_rows, HEADS, HEAD)
    key_heads = keys_local.reshape(-1, HEADS, HEAD)
    value_heads = values_local.reshape(-1, HEADS, HEAD)
    scores = (
        jnp.einsum("qhd,khd->hqk", query_heads, key_heads, preferred_element_type=jnp.float32)
        * scale
    )
    scores = jnp.where(live_local[None, None, :], scores, -1e30)
    local_top = jnp.max(scores, axis=2)
    global_top = lax.pmax(local_top, "seq")
    weights = jnp.where(live_local[None, None, :], jnp.exp(scores - global_top[:, :, None]), 0.0)
    totals = jnp.sum(weights, axis=2)
    summed = jnp.einsum(
        "hqk,khd->qhd",
        weights.astype(jnp.bfloat16),
        value_heads,
        preferred_element_type=jnp.float32,
    )
    own_sums, own_totals = (
        lax.psum_scatter(summed.reshape(total_rows, width), "seq", scatter_dimension=0, tiled=True),
        lax.psum_scatter(totals.T, "seq", scatter_dimension=0, tiled=True),
    )
    mixed = (
        (own_sums.reshape(own_rows, HEADS, HEAD) / own_totals[:, :, None])
        .reshape(own_rows, width)
        .astype(jnp.bfloat16)
    )
    projected = jnp.dot(mixed, attn_out_weight, preferred_element_type=jnp.float32)
    onehot = (
        timestep[:, None] == jnp.arange(gate_table.shape[0], dtype=jnp.int32)[None, :]
    ).astype(jnp.float32)
    gate = jnp.dot(onehot, gate_table, precision=lax.Precision.HIGHEST)
    stream_out = (stream[0].astype(jnp.float32) + gate * projected).astype(jnp.bfloat16)[None]
    grad_in, grad_weight = critic_pass(critic_in, critic_cot, critic_weight)
    return (stream_out, grad_in, grad_weight)


def step_kernel(
    zs,
    parts,
    stream_hbm,
    queries,
    new_keys,
    new_values,
    cache_keys,
    cache_values,
    frames_hbm,
    group_hbm,
    timestep_hbm,
    gate_hbm,
    out_weight_hbm,
    critic_in,
    critic_cot,
    weight_hbm,
    stream_out,
    grad_in,
    grad_weight,
    cot,
    wdiag,
    cin,
    out_weight,
    wfull,
    gmine,
    psend,
    precv,
    dsend,
    xsend,
    ysend,
    rdiag,
    rx,
    ry,
    osum,
    zsend,
    zrecv,
    q_all,
    q_other,
    kfull,
    vfull,
    frames,
    live_row,
    asend,
    arecv,
    mixed,
    stream,
    gate_table,
    group_index,
    timestep,
    send_sems,
    recv_sems,
    local_sems,
):
    f32, bf16 = jnp.float32, jnp.bfloat16
    dp, seq = lax.axis_index("dp"), lax.axis_index("seq")
    z, core = seq // 2, lax.rem(seq, 2)
    other = 1 - core
    tokens, width = cin.shape
    block = width // 4
    half = width // 2
    own_q = queries.shape[0]
    cached, fresh = cache_keys.shape[0], new_keys.shape[0]
    keys_one = cached + fresh
    heads_here = half // HEAD
    zh = zs // 2
    dp_x = dp + 1 - 2 * lax.rem(dp, 2)
    dp_y = lax.rem(dp + 2, 4)
    dp_d = dp_x + 2 - 4 * (dp_x // 2)
    order = (dp_d, dp_x, dp_y, dp)
    xn, yn, pair = (dp_x, seq), (dp_y, seq), (dp, z * 2 + other)

    near = z + 1 - 2 * lax.rem(z, 2)
    across = zs - 1 - z
    far = zs - 1 - near
    inner = (z == 1) | (z == 2)
    to_near, to_across = (dp, near * 2 + core), (dp, across * 2 + core)
    second = jnp.where(inner, across, far)
    third = jnp.where(inner, far, across)
    held = (z, near, second, third)

    other_cols = pl.ds(pl.multiple_of(other * half, 128), half)
    own_cols = pl.ds(pl.multiple_of(core * half, 128), half)

    started = []

    def load(src, dst):
        copy = pltpu.make_async_copy(src, dst, local_sems.at[len(started)])
        copy.start()
        started.append(copy)
        return copy

    def columns(b):
        return pl.ds(pl.multiple_of(order[b] * block, 128), block)

    weight_load = load(weight_hbm, wfull.at[dp, z, core])
    q_load = load(queries.at[:, own_cols], q_all.at[seq])
    q_other_load = load(queries.at[:, other_cols], q_other)
    cot_load = load(critic_cot, cot)
    cin_loads = [load(critic_in.at[:, columns(b)], cin.at[:, columns(b)]) for b in range(4)]
    small_loads = [
        load(cache_keys.at[:, own_cols], kfull.at[pl.ds(0, cached)]),
        load(new_keys.at[:, own_cols], kfull.at[pl.ds(cached, fresh)]),
        load(cache_values.at[:, own_cols], vfull.at[pl.ds(0, cached)]),
        load(new_values.at[:, own_cols], vfull.at[pl.ds(cached, fresh)]),
        load(frames_hbm, frames.at[0]),
        load(group_hbm, group_index),
        load(timestep_hbm, timestep),
        load(gate_hbm, gate_table),
        load(stream_hbm, stream),
        load(out_weight_hbm, out_weight),
    ]

    barrier = pltpu.get_barrier_semaphore()
    peers = [xn, yn, pair]
    for j in range(1, zs):
        zt = lax.rem(z + j, zs)
        peers += [(dp, zt * 2 + core), (dp, zt * 2 + other)]
    for peer in peers:
        pl.semaphore_signal(
            barrier, inc=1, device_id=peer, device_id_type=pl.DeviceIdType.MESH
        )
    pl.semaphore_wait(barrier, len(peers))

    sent = []

    def remote(src, dst, slot, peer, n):
        return pltpu.make_async_remote_copy(
            src_ref=src,
            dst_ref=dst,
            send_sem=send_sems.at[n],
            recv_sem=recv_sems.at[slot],
            device_id=peer,
            device_id_type=pl.DeviceIdType.MESH,
        )

    def send(src, dst, slot, peer, when=None):
        copy = remote(src, dst, slot, peer, len(sent))
        if when is None:
            copy.start()
        else:
            pl.when(when)(copy.start)
        sent.append((copy, when))

    def arrived(dst, slot):
        remote(dst, dst, slot, pair, 0).wait_recv()

    W_Z, W_X, W_Y, W_P = 0, zs, 2 * zs, 3 * zs
    W_PX, W_PY, W_D, W_PD = 4 * zs, 5 * zs, 6 * zs, 7 * zs
    Q_Z, KV_P = 8 * zs, 10 * zs
    G_P = 10 * zs + 5
    G_D, G_X, G_Y, G_Z = G_P + 4 * zs, G_P + 5 * zs, G_P + 6 * zs, G_P + 7 * zs
    A_Z = G_P + 8 * zs

    q_load.wait()
    q_other_load.wait()
    for chip, when in ((near, None), (across, inner)):
        send(q_all.at[seq], q_all.at[seq], Q_Z + seq, (dp, chip * 2 + core), when)
        send(q_other, q_all.at[seq], Q_Z + seq, (dp, chip * 2 + other), when)
    send(q_other, q_all.at[seq], Q_Z + seq, pair)
    mine = wfull.at[dp, z, core]
    weight_load.wait()
    send(mine, mine, W_Z + z, to_near)
    send(mine, mine, W_Z + z, to_across, inner)
    send(mine, mine, W_X, xn)
    send(mine, mine, W_Y, yn)
    send(mine, mine, W_P, pair)

    def grad_block(b):
        cin_loads[b].wait()
        acc = lax.dot_general(
            cin[:, columns(b)],
            cot[...],
            (((0,), (0,)), ((), ())),
            preferred_element_type=f32,
        )
        shard = block // (2 * zs)
        for k in range(zs):
            lo = acc[2 * k * shard : (2 * k + 1) * shard]
            hi = acc[(2 * k + 1) * shard : (2 * k + 2) * shard]
            gmine[b, k] = jnp.where(core == 0, lo, hi)
            psend[b, k] = jnp.where(core == 0, hi, lo).astype(bf16)
        for k in range(zs):
            send(psend.at[b, k], precv.at[b, k], G_P + b * zs + k, pair)

    def chip_sum(b, k):
        arrived(precv.at[b, k], G_P + b * zs + k)
        return gmine[b, k] + precv[b, k].astype(f32)

    cot_load.wait()
    grad_block(0)

    grad_block(1)
    for k in (0, 3, 1, 2):
        dsend[k] = chip_sum(0, k).astype(bf16)
        send(dsend.at[k], rdiag.at[k], G_D + k, xn if k < zh else yn)
    grad_block(2)

    def send_x(k):
        total = chip_sum(1, k)
        if k >= zh:
            arrived(rdiag.at[k], G_D + k)
            total = total + rdiag[k].astype(f32)
        xsend[k] = total.astype(bf16)
        send(xsend.at[k], rx.at[k], G_X + k, xn)

    def send_y(k):
        total = chip_sum(2, k)
        if k < zh:
            arrived(rdiag.at[k], G_D + k)
            total = total + rdiag[k].astype(f32)
        ysend[k] = total.astype(bf16)
        send(ysend.at[k], ry.at[k], G_Y + k, yn)

    def line(of):
        def take(source):
            for ref, slot in of(source):
                arrived(ref, slot)

        def pass_on(source, peer):
            for ref, slot in of(source):
                send(ref, ref, slot, peer, inner)

        def first():
            take(near)
            pass_on(near, to_across)

        def inner_second():
            pl.when(inner)(lambda: take(across))
            pass_on(across, to_near)

        def both_third():
            take(far)
            pass_on(far, to_near)

        def outer_last():
            pl.when(jnp.logical_not(inner))(lambda: take(across))

        return first, inner_second, both_third, outer_last

    w_line = line(lambda s: [(wfull.at[dp, s, core], W_Z + s)])
    q_line = line(lambda s: [(q_all.at[2 * s + c], Q_Z + 2 * s + c) for c in range(2)])

    q_line[0]()
    q_line[1]()
    send_x(0)
    send_y(3)
    w_line[0]()
    w_line[1]()
    grad_block(3)
    q_line[2]()
    send(cache_keys.at[:, other_cols], kfull.at[pl.ds(keys_one, cached)], KV_P, pair)
    send(new_keys.at[:, other_cols], kfull.at[pl.ds(keys_one + cached, fresh)], KV_P + 1, pair)
    send(cache_values.at[:, other_cols], vfull.at[pl.ds(keys_one, cached)], KV_P + 2, pair)
    send(new_values.at[:, other_cols], vfull.at[pl.ds(keys_one + cached, fresh)], KV_P + 3, pair)
    send(frames_hbm, frames.at[1], KV_P + 4, pair)

    def attention():
        arrived(kfull.at[pl.ds(keys_one, cached)], KV_P)
        arrived(kfull.at[pl.ds(keys_one + cached, fresh)], KV_P + 1)
        arrived(vfull.at[pl.ds(keys_one, cached)], KV_P + 2)
        arrived(vfull.at[pl.ds(keys_one + cached, fresh)], KV_P + 3)
        arrived(frames.at[1], KV_P + 4)
        for copy in small_loads:
            copy.wait()
        first_frame = FRAMES_GROUP * group_index[0]
        live_row[...] = jnp.ones_like(live_row)
        for at, which in ((0, 0), (keys_one, 1)):
            f = frames[which]
            ok = (f < first_frame) & (f >= first_frame - WINDOW_FRAMES)
            live_row[:, at : at + cached] = jnp.where(ok, 1.0, 0.0)
        live = live_row[...] > 0.5
        rows_q = 2 * zs * own_q
        lane = lax.broadcasted_iota(jnp.int32, (rows_q, 128), 1)
        stats = jnp.zeros((rows_q, 128), f32)
        for h in range(heads_here):
            cols = slice(h * HEAD, (h + 1) * HEAD)
            q_head = q_all[:, :, cols].reshape(rows_q, HEAD)
            scores = lax.dot_general(
                q_head, kfull[:, cols], (((1,), (1,)), ((), ())), preferred_element_type=f32
            ) * (HEAD ** (-0.5))
            scores = jnp.where(live, scores, -1e30)
            top = jnp.max(scores, axis=1, keepdims=True)
            weights = jnp.where(live, jnp.exp(scores - top), 0.0)
            total = jnp.sum(weights, axis=1, keepdims=True)
            summed = jnp.dot(weights.astype(bf16), vfull[:, cols], preferred_element_type=f32)
            asend[:, :, cols] = summed.astype(bf16).reshape(2 * zs, own_q, HEAD)
            for at, value in ((0, top), (64, total)):
                for part in range(3):
                    piece = value.astype(bf16).astype(f32)
                    stats = jnp.where(lane == at + 16 * part + h, piece, stats)
                    value = value - piece
        asend[:, :, half:] = stats.astype(bf16).reshape(2 * zs, own_q, 128)
        for zt in (near, second, third):
            for ct in (core, other):
                at = zt * 2 + ct
                send(asend.at[at], arecv.at[seq], A_Z + seq, (dp, at))
        send(asend.at[z * 2 + other], arecv.at[seq], A_Z + seq, pair)
        arecv[seq] = asend[seq]

    send_y(0)
    send_x(3)
    send_x(1)
    send_y(2)
    w_line[2]()
    arrived(q_all.at[z * 2 + other], Q_Z + z * 2 + other)
    q_line[3]()
    attention()
    send_y(1)
    send_x(2)

    def w_out(j):
        shard_ref = wfull.at[dp, held[j], core]
        send(shard_ref, shard_ref, W_X + j, xn)
        send(shard_ref, shard_ref, W_Y + j, yn)
        send(shard_ref, shard_ref, W_P + j, pair)

    w_out(1)
    w_line[3]()
    w_out(2)
    w_out(3)

    def grad_in_block(b):
        rows = wfull[order[b]].reshape(block, width)
        step = 512

        def body(t, carry):
            at = pl.ds(pl.multiple_of(t * step, step), step)
            grad_in[at, columns(b)] = lax.dot_general(
                cot[at], rows, (((1,), (1,)), ((), ())), preferred_element_type=f32
            ).astype(bf16)
            return carry

        lax.fori_loop(0, tokens // step, body, 0)

    for j in range(zs):
        arrived(wfull.at[dp, held[j], other], W_P + j)
    grad_in_block(3)

    for k in (0, 3, 1, 2):
        arrived(rx.at[k], G_X + k)
        arrived(ry.at[k], G_Y + k)
        osum[k] = chip_sum(3, k) + rx[k].astype(f32) + ry[k].astype(f32)

        @pl.when(z != k)
        def _():
            zsend[k] = osum[k].astype(bf16)

        send(zsend.at[k], zrecv.at[z], G_Z + z, (dp, 2 * k + core), z != k)

    def from_sides(j):
        arrived(wfull.at[dp_x, held[j], core], W_X + j)
        shard_ref = wfull.at[dp_x, held[j], core]
        if j < zh:
            send(shard_ref, wdiag.at[held[j], core], W_D + j, yn)
        send(shard_ref, shard_ref, W_PX + j, pair)
        arrived(wfull.at[dp_y, held[j], core], W_Y + j)
        shard_ref = wfull.at[dp_y, held[j], core]
        if j >= zh:
            send(shard_ref, wdiag.at[held[j], core], W_D + j, xn)
        send(shard_ref, shard_ref, W_PY + j, pair)

    def grad_in_sides():
        for j in range(zs):
            arrived(wfull.at[dp_x, held[j], other], W_PX + j)
            arrived(wfull.at[dp_y, held[j], other], W_PY + j)
        rows = jnp.concatenate(
            [wfull[dp_x].reshape(block, width), wfull[dp_y].reshape(block, width)]
        )
        step = 512

        def body(t, carry):
            at = pl.ds(pl.multiple_of(t * step, step), step)
            both = lax.dot_general(
                cot[at], rows, (((1,), (1,)), ((), ())), preferred_element_type=f32
            ).astype(bf16)
            grad_in[at, columns(1)] = both[:, :block]
            grad_in[at, columns(2)] = both[:, block:]
            return carry

        lax.fori_loop(0, tokens // step, body, 0)

    def attention_out():
        for zt in (near, second, third):
            for ct in (core, other):
                arrived(arecv.at[zt * 2 + ct], A_Z + zt * 2 + ct)
        arrived(arecv.at[z * 2 + other], A_Z + z * 2 + other)

        def stat(zt, ct, at, h):
            s = arecv[zt * 2 + ct, :, half:].astype(f32)
            return s[:, at + h : at + h + 1] + (
                s[:, at + 16 + h : at + 17 + h] + s[:, at + 32 + h : at + 33 + h]
            )

        for ct in range(2):
            for h in range(heads_here):
                cols = slice(h * HEAD, (h + 1) * HEAD)
                tops = [stat(zt, ct, 0, h) for zt in range(zs)]
                sums = [stat(zt, ct, 64, h) for zt in range(zs)]
                top = functools.reduce(jnp.maximum, tops)
                acc = jnp.zeros((own_q, HEAD), f32)
                total = jnp.zeros((own_q, 1), f32)
                for zt in range(zs):
                    scale = jnp.exp(tops[zt] - top)
                    acc = acc + scale * arecv[zt * 2 + ct, :, cols].astype(f32)
                    total = total + scale * sums[zt]
                mixed[:, ct * half + h * HEAD : ct * half + (h + 1) * HEAD] = (acc / total).astype(bf16)
        gate = jnp.zeros((1, width), f32)
        for s in range(gate_table.shape[0]):
            gate = gate + jnp.where(timestep[0] == s, gate_table[s : s + 1], 0.0)
        projected = jnp.dot(mixed[...], out_weight[...], preferred_element_type=f32)
        stream_out[...] = (stream[...].astype(f32) + gate * projected).astype(bf16)
    from_sides(0)
    from_sides(1)
    from_sides(2)
    attention_out()
    from_sides(3)

    grad_in_sides()
    for j in range(zs):
        shard_ref = wdiag.at[held[j], core]
        arrived(shard_ref, W_D + j)
        send(shard_ref, shard_ref, W_PD + j, pair)

    factor = float(tokens * parts) ** (-0.5)
    grad = osum[z]
    for zt in (near, second, third):
        arrived(zrecv.at[zt], G_Z + zt)
        grad = grad + zrecv[zt].astype(f32)
    grad_weight[...] = grad * factor

    for j in range(zs):
        arrived(wdiag.at[held[j], other], W_PD + j)

    for copy, when in sent:
        if when is None:
            copy.wait_send()
        else:
            pl.when(when)(copy.wait_send)


def finish_kernel(
    stream_part,
    grad_part,
    weight_part,
    cot,
    wdiag,
    stream_out,
    grad_in,
    grad_weight,
    last,
    sems,
):
    tokens, width = cot.shape
    block = width // 4
    dp = lax.axis_index("dp")
    dp_x = dp + 1 - 2 * lax.rem(dp, 2)
    dp_y = lax.rem(dp + 2, 4)
    dp_d = dp_x + 2 - 4 * (dp_x // 2)
    copies = []

    def put(src, dst):
        copy = pltpu.make_async_copy(src, dst, sems.at[len(copies)])
        copy.start()
        copies.append(copy)

    def columns(b):
        return pl.ds(pl.multiple_of(b * block, 128), block)

    for b in (dp, dp_x, dp_y):
        put(grad_part.at[:, columns(b)], grad_in.at[:, columns(b)])
    put(stream_part, stream_out)
    put(weight_part, grad_weight)
    rows = wdiag[...].reshape(block, width)
    pieces = 4
    step = tokens // pieces
    for t in range(pieces):
        at = slice(t * step, (t + 1) * step)
        last[at] = lax.dot_general(
            cot[at], rows, (((1,), (1,)), ((), ())), preferred_element_type=jnp.float32
        ).astype(last.dtype)
        put(last.at[at], grad_in.at[at, columns(dp_d)])
    for copy in copies:
        copy.wait()


def fused(
    stream,
    queries,
    new_keys,
    new_values,
    cache_keys,
    cache_values,
    cache_frames,
    group_index,
    timestep,
    gate_table,
    attn_out_weight,
    critic_in,
    critic_cot,
    critic_weight,
):
    bf16, f32 = jnp.bfloat16, jnp.float32
    zs = lax.axis_size("seq") // 2
    parts = lax.axis_size(("dp", "seq"))
    tokens, width = critic_in.shape
    own_q = queries.shape[1]
    shard = critic_weight.shape[0]
    cached, fresh = cache_keys.shape[1], new_keys.shape[1]
    half = width // 2
    keys_two = 2 * (cached + fresh)
    vmem, smem = pltpu.VMEM, pltpu.SMEM
    hbm = pl.BlockSpec(memory_space=pltpu.HBM)
    shards = (zs, shard, width)
    parts_out = pl.pallas_call(
        functools.partial(step_kernel, zs, parts),
        out_shape=(
            vmem((own_q, width), bf16),
            vmem((tokens, width), bf16),
            vmem((shard, width), f32),
            vmem((tokens, width), bf16),
            vmem((zs, 2, shard, width), bf16),
        ),
        in_specs=[hbm] * 14,
        out_specs=(pl.BlockSpec(memory_space=vmem),) * 5,
        scratch_shapes=[
            vmem((tokens, width), bf16),
            vmem((width, width), bf16),
            vmem((4, zs, 2, shard, width), bf16),
            vmem((4,) + shards, f32),
            vmem((4,) + shards, bf16),
            vmem((4,) + shards, bf16),
            vmem(shards, bf16),
            vmem(shards, bf16),
            vmem(shards, bf16),
            vmem(shards, bf16),
            vmem(shards, bf16),
            vmem(shards, bf16),
            vmem(shards, f32),
            vmem(shards, bf16),
            vmem(shards, bf16),
            vmem((2 * zs, own_q, half), bf16),
            vmem((own_q, half), bf16),
            vmem((keys_two, half), bf16),
            vmem((keys_two, half), bf16),
            vmem((2, 1, cached), jnp.int32),
            vmem((1, keys_two), f32),
            vmem((2 * zs, own_q, half + 128), bf16),
            vmem((2 * zs, own_q, half + 128), bf16),
            vmem((own_q, width), bf16),
            vmem((own_q, width), bf16),
            vmem(gate_table.shape, f32),
            smem((1,), jnp.int32),
            smem((1,), jnp.int32),
            pltpu.SemaphoreType.DMA((120,)),
            pltpu.SemaphoreType.DMA((20 * zs + 5,)),
            pltpu.SemaphoreType.DMA((18,)),
        ],
        compiler_params=pltpu.CompilerParams(
            collective_id=0, has_side_effects=True, vmem_limit_bytes=VMEM_LIMIT
        ),
    )(
        *(
            a if a.shape == (1,) else pltpu.with_memory_space_constraint(a, pltpu.HBM)
            for a in (
                stream[0],
                queries[0],
                new_keys[0],
                new_values[0],
                cache_keys[0],
                cache_values[0],
                cache_frames,
                group_index,
                timestep,
                gate_table,
                attn_out_weight,
                critic_in,
                critic_cot,
                critic_weight,
            )
        )
    )
    stream_out, grad_in, grad_weight = pl.pallas_call(
        finish_kernel,
        out_shape=(
            jax.ShapeDtypeStruct((own_q, width), bf16),
            jax.ShapeDtypeStruct((tokens, width), bf16),
            jax.ShapeDtypeStruct((shard, width), f32),
        ),
        in_specs=[pl.BlockSpec(memory_space=vmem)] * 5,
        out_specs=(hbm,) * 3,
        scratch_shapes=[
            vmem((tokens, width // 4), bf16),
            pltpu.SemaphoreType.DMA((9,)),
        ],
        compiler_params=pltpu.CompilerParams(vmem_limit_bytes=FINISH_LIMIT),
    )(*(pltpu.with_memory_space_constraint(a, vmem) for a in parts_out))
    return (stream_out[None], grad_in, grad_weight)


def local(*args):
    shard, tokens = args[13].shape[0], args[11].shape[0]
    fits = (
        lax.axis_size("dp") == 4
        and lax.axis_size("seq") == 8
        and shard % 16 == 0
        and args[1].shape[1] % 16 == 0
        and args[4].shape[1] % 16 == 0
        and args[1].shape[2] % 512 == 0
        and tokens % 256 == 0
    )
    return fused(*args) if fits else by_collectives(*args)


def solution(mesh):
    return jax.shard_map(
        local,
        mesh=mesh,
        in_specs=(
            P("dp", "seq", None),
            P("dp", "seq", None),
            P("dp", "seq", None),
            P("dp", "seq", None),
            P("dp", "seq", None),
            P("dp", "seq", None),
            P("dp", "seq"),
            P("dp"),
            P("dp"),
            P(),
            P(),
            P(("dp", "seq"), None),
            P(("dp", "seq"), None),
            P(("dp", "seq"), None),
        ),
        out_specs=(P("dp", "seq", None), P(("dp", "seq"), None), P(("dp", "seq"), None)),
        check_vma=False,
    )
```

```python
import functools

import jax
import jax.numpy as jnp
from jax import lax
from jax.experimental import pallas as pl
from jax.experimental.pallas import tpu as pltpu
from jax.sharding import PartitionSpec as P

HEADS = 12
HEAD = 128
FRAMES_GROUP = 3
WINDOW_FRAMES = 9
VMEM_LIMIT = 44 * 1024 * 1024
EARLY = 128
FINISH_LIMIT = 8 * 1024 * 1024


def critic_pass(critic_in, critic_cot, critic_weight):
    grad_in = lax.dot_general(
        critic_cot,
        lax.all_gather(critic_weight, ("dp", "seq"), axis=0, tiled=True),
        (((1,), (1,)), ((), ())),
        preferred_element_type=jnp.float32,
    ).astype(jnp.bfloat16)
    factor = float(critic_in.shape[0] * lax.axis_size(("dp", "seq"))) ** (-0.5)
    whole_term = (
        lax.dot_general(
            critic_in, critic_cot, (((0,), (0,)), ((), ())), preferred_element_type=jnp.float32
        )
        * factor
    )
    grad_weight = lax.psum_scatter(whole_term, ("dp", "seq"), scatter_dimension=0, tiled=True)
    return (grad_in, grad_weight)


def by_collectives(
    stream,
    queries,
    new_keys,
    new_values,
    cache_keys,
    cache_values,
    cache_frames,
    group_index,
    timestep,
    gate_table,
    attn_out_weight,
    critic_in,
    critic_cot,
    critic_weight,
):
    query_local = queries[0]
    own_rows = query_local.shape[0]
    width = query_local.shape[1]
    scale = HEAD ** (-0.5)
    first_frame = FRAMES_GROUP * group_index[0]
    frames = cache_frames[0]
    live_cache = (frames < first_frame) & (frames >= first_frame - WINDOW_FRAMES)
    live_local = jnp.concatenate([live_cache, jnp.ones((own_rows,), dtype=bool)])
    keys_local = jnp.concatenate([cache_keys[0], new_keys[0]], axis=0)
    values_local = jnp.concatenate([cache_values[0], new_values[0]], axis=0)
    all_queries = lax.all_gather(queries, "seq", axis=1, tiled=True)[0]
    total_rows = all_queries.shape[0]
    query_heads = all_queries.reshape(total_rows, HEADS, HEAD)
    key_heads = keys_local.reshape(-1, HEADS, HEAD)
    value_heads = values_local.reshape(-1, HEADS, HEAD)
    scores = (
        jnp.einsum("qhd,khd->hqk", query_heads, key_heads, preferred_element_type=jnp.float32)
        * scale
    )
    scores = jnp.where(live_local[None, None, :], scores, -1e30)
    local_top = jnp.max(scores, axis=2)
    global_top = lax.pmax(local_top, "seq")
    weights = jnp.where(live_local[None, None, :], jnp.exp(scores - global_top[:, :, None]), 0.0)
    totals = jnp.sum(weights, axis=2)
    summed = jnp.einsum(
        "hqk,khd->qhd",
        weights.astype(jnp.bfloat16),
        value_heads,
        preferred_element_type=jnp.float32,
    )
    own_sums, own_totals = (
        lax.psum_scatter(summed.reshape(total_rows, width), "seq", scatter_dimension=0, tiled=True),
        lax.psum_scatter(totals.T, "seq", scatter_dimension=0, tiled=True),
    )
    mixed = (
        (own_sums.reshape(own_rows, HEADS, HEAD) / own_totals[:, :, None])
        .reshape(own_rows, width)
        .astype(jnp.bfloat16)
    )
    projected = jnp.dot(mixed, attn_out_weight, preferred_element_type=jnp.float32)
    onehot = (
        timestep[:, None] == jnp.arange(gate_table.shape[0], dtype=jnp.int32)[None, :]
    ).astype(jnp.float32)
    gate = jnp.dot(onehot, gate_table, precision=lax.Precision.HIGHEST)
    stream_out = (stream[0].astype(jnp.float32) + gate * projected).astype(jnp.bfloat16)[None]
    grad_in, grad_weight = critic_pass(critic_in, critic_cot, critic_weight)
    return (stream_out, grad_in, grad_weight)


def step_kernel(
    zs,
    parts,
    stream_hbm,
    queries,
    new_keys,
    new_values,
    cache_keys,
    cache_values,
    frames_hbm,
    group_hbm,
    timestep_hbm,
    gate_hbm,
    out_weight_hbm,
    critic_in,
    critic_cot,
    weight_hbm,
    stream_out,
    grad_in,
    grad_weight,
    cot,
    wdiag,
    cin,
    out_weight,
    wfull,
    gmine,
    psend,
    precv,
    dsend,
    xsend,
    ysend,
    rdiag,
    rx,
    ry,
    osum,
    zsend,
    zrecv,
    chain,
    q_all,
    q_other,
    kfull,
    vfull,
    frames,
    live_row,
    asend,
    arecv,
    mixed,
    stream,
    gate_table,
    group_index,
    timestep,
    send_sems,
    recv_sems,
    local_sems,
):
    f32, bf16 = jnp.float32, jnp.bfloat16
    dp, seq = lax.axis_index("dp"), lax.axis_index("seq")
    z, core = seq // 2, lax.rem(seq, 2)
    other = 1 - core
    tokens, width = cin.shape
    block = width // 4
    half = width // 2
    whole, early = pl.ds(0, width), pl.ds(width - EARLY, EARLY)
    late = pl.ds(0, width - EARLY)
    own_q = queries.shape[0]
    cached, fresh = cache_keys.shape[0], new_keys.shape[0]
    keys_one = cached + fresh
    heads_here = half // HEAD
    zh = zs // 2
    dp_x = dp + 1 - 2 * lax.rem(dp, 2)
    dp_y = lax.rem(dp + 2, 4)
    dp_d = dp_x + 2 - 4 * (dp_x // 2)
    order = (dp_d, dp_x, dp_y, dp)
    xn, yn, pair = (dp_x, seq), (dp_y, seq), (dp, z * 2 + other)

    near = z + 1 - 2 * lax.rem(z, 2)
    across = zs - 1 - z
    far = zs - 1 - near
    inner = (z == 1) | (z == 2)
    outer = jnp.logical_not(inner)
    to_near, to_across = (dp, near * 2 + core), (dp, across * 2 + core)
    second = jnp.where(inner, across, far)
    third = jnp.where(inner, far, across)
    held = (z, near, second, third)

    other_cols = pl.ds(pl.multiple_of(other * half, 128), half)
    own_cols = pl.ds(pl.multiple_of(core * half, 128), half)

    started = []

    def load(src, dst):
        copy = pltpu.make_async_copy(src, dst, local_sems.at[len(started)])
        copy.start()
        started.append(copy)
        return copy

    def columns(b):
        return pl.ds(pl.multiple_of(order[b] * block, 128), block)

    weight_load = load(weight_hbm, wfull.at[dp, z, core])
    q_load = load(queries.at[:, own_cols], q_all.at[seq])
    q_other_load = load(queries.at[:, other_cols], q_other)
    cot_load = load(critic_cot, cot)
    cin_loads = [load(critic_in.at[:, columns(b)], cin.at[:, columns(b)]) for b in range(4)]
    small_loads = [
        load(cache_keys.at[:, own_cols], kfull.at[pl.ds(0, cached)]),
        load(new_keys.at[:, own_cols], kfull.at[pl.ds(cached, fresh)]),
        load(cache_values.at[:, own_cols], vfull.at[pl.ds(0, cached)]),
        load(new_values.at[:, own_cols], vfull.at[pl.ds(cached, fresh)]),
        load(frames_hbm, frames.at[0]),
        load(group_hbm, group_index),
        load(timestep_hbm, timestep),
        load(gate_hbm, gate_table),
        load(stream_hbm, stream),
        load(out_weight_hbm, out_weight),
    ]

    barrier = pltpu.get_barrier_semaphore()
    peers = [xn, yn, pair]
    for j in range(1, zs):
        zt = lax.rem(z + j, zs)
        peers += [(dp, zt * 2 + core), (dp, zt * 2 + other)]
    for peer in peers:
        pl.semaphore_signal(
            barrier, inc=1, device_id=peer, device_id_type=pl.DeviceIdType.MESH
        )
    pl.semaphore_wait(barrier, len(peers))

    groups = {}

    def remote(src, dst, slot, peer, n):
        return pltpu.make_async_remote_copy(
            src_ref=src,
            dst_ref=dst,
            send_sem=send_sems.at[n],
            recv_sem=recv_sems.at[slot],
            device_id=peer,
            device_id_type=pl.DeviceIdType.MESH,
        )

    def send(src, dst, slot, peer, group, when=None):
        n = groups.setdefault(group, len(groups))
        copy = remote(src, dst, slot, peer, n)
        if when is None:
            copy.start()
        else:
            pl.when(when)(copy.start)

    def all_sent():
        eight = precv.at[pl.ds(0, 2)]
        twelve = precv.at[pl.ds(0, 3)]
        three = pl.ds(0, 3)
        totals = {
            "own": (eight, None),
            "one": (precv.at[0, 0], None),
            "line": (precv.at[0], inner),
            "psend": (precv, None),
            "sums": (twelve, None),
            "late": (precv.at[:, :, :, late], None),
            "diag": (precv.at[0, :, :, late], None),
            "chip1": (precv.at[0, 0], z != 1),
            "chip2": (precv.at[0, 0], z != 2),
            "start": (precv.at[0, 0], outer),
            "far": (precv.at[0, 0], inner),
            "near": (precv.at[0, 0], inner),
            "early": (precv.at[three, :, :, early], None),
            "early0": (precv.at[0, 0, :, early], None),
            "earlyd": (precv.at[0, 0, :, early], None),
            "fline": (precv.at[three, :, :, early], inner),
            "q": (q_all.at[three], None),
            "qline": (q_all, inner),
            "k": (kfull.at[pl.ds(0, keys_one)], None),
            "v": (vfull.at[pl.ds(0, keys_one)], None),
            "frames": (frames.at[0], None),
            "parts": (arecv.at[pl.ds(0, 2 * zs - 1)], None),
        }
        for group, n in groups.items():
            view, when = totals[group]
            wait = remote(view, view, 0, pair, n).wait_send
            if when is None:
                wait()
            else:
                pl.when(when)(wait)

    def arrived(dst, slot):
        remote(dst, dst, slot, pair, 0).wait_recv()

    W_Z, W_X, W_Y, F_Z, Q_Z = 0, zs, 2 * zs, 3 * zs, 4 * zs
    G_P, G_D, G_X, G_Y = 6 * zs, 10 * zs, 11 * zs, 12 * zs
    W_P, W_PX, W_PY, W_PD, W_D, F_OWN = (13 * zs + i for i in range(6))
    K_P, V_P, FRAMES_P, A_Z, G_Z = (13 * zs + 6 + i for i in range(5))
    C_FAR, C_MID, C_END = (13 * zs + 11 + i for i in range(3))

    q_load.wait()
    q_other_load.wait()
    for chip, when in ((near, None), (across, inner)):
        send(q_all.at[seq], q_all.at[seq], Q_Z + seq, (dp, chip * 2 + core), "qline" if when is not None else "q", when)
        send(q_other, q_all.at[seq], Q_Z + seq, (dp, chip * 2 + other), "qline" if when is not None else "q", when)
    send(q_other, q_all.at[seq], Q_Z + seq, pair, "q")
    mine = wfull.at[dp, z, core]
    weight_load.wait()
    send(mine, mine, W_Z + z, to_near, "own")
    send(mine, mine, W_Z + z, to_across, "line", inner)
    send(mine, mine, W_X, xn, "own")
    send(mine, mine, W_Y, yn, "own")
    send(mine, mine, W_P, pair, "own")

    def grad_block(b):
        cin_loads[b].wait()
        acc = lax.dot_general(
            cin[:, columns(b)],
            cot[...],
            (((0,), (0,)), ((), ())),
            preferred_element_type=f32,
        )
        shard = block // (2 * zs)
        for k in range(zs):
            lo = acc[2 * k * shard : (2 * k + 1) * shard]
            hi = acc[(2 * k + 1) * shard : (2 * k + 2) * shard]
            gmine[b, k] = jnp.where(core == 0, lo, hi)
            psend[b, k] = jnp.where(core == 0, hi, lo).astype(bf16)
        for k in range(zs):
            send(psend.at[b, k], precv.at[b, k], G_P + b * zs + k, pair, "psend")

    def chip_sum(b, k):
        arrived(precv.at[b, k], G_P + b * zs + k)
        return gmine[b, k] + precv[b, k].astype(f32)

    cot_load.wait()
    grad_block(0)

    def send_x(k):
        total = chip_sum(1, k)
        if k >= zh:
            arrived(rdiag.at[k], G_D + k)
            total = total + rdiag[k].astype(f32)
        xsend[k] = total.astype(bf16)
        send(xsend.at[k], rx.at[k], G_X + k, xn, "sums")

    def send_y(k):
        total = chip_sum(2, k)
        if k < zh:
            arrived(rdiag.at[k], G_D + k)
            total = total + rdiag[k].astype(f32)
        ysend[k] = total.astype(bf16)
        send(ysend.at[k], ry.at[k], G_Y + k, yn, "sums")

    def line(of, group):
        def take(source):
            if group == "fline":
                arrived(precv.at[0, pl.ds(0, 3), :, early], F_Z + source)
                return
            for ref, slot in of(source):
                arrived(ref, slot)

        def pass_on(source, peer):
            for ref, slot in of(source):
                send(ref, ref, slot, peer, group, inner)

        def first():
            take(near)
            pass_on(near, to_across)

        def inner_second():
            pl.when(inner)(lambda: take(across))
            pass_on(across, to_near)

        def both_third():
            take(far)
            pass_on(far, to_near)

        def outer_last():
            pl.when(outer)(lambda: take(across))

        def inner_third():
            pl.when(inner)(lambda: take(far))
            pass_on(far, to_near)

        def outer_third():
            pl.when(outer)(lambda: take(far))

        return first, inner_second, both_third, outer_last, inner_third, outer_third

    def early_pieces(s, c):
        return [
            (wfull.at[dp_x, s, c, :, early], F_Z + s),
            (wfull.at[dp_y, s, c, :, early], F_Z + s),
            (wdiag.at[s, c, :, early], F_Z + s),
        ]

    def early_diag():
        arrived(wfull.at[dp_x, z, core], W_X)
        arrived(wfull.at[dp_y, z, core], W_Y)
        for way, peer, when in ((dp_x, yn, core == 0), (dp_y, xn, core == 1)):
            send(
                wfull.at[way, z, core, :, early], wdiag.at[z, core, :, early], F_OWN, peer, "earlyd", when
            )

    def early_own():
        arrived(wdiag.at[z, core, :, early], F_OWN)
        for ref, slot in early_pieces(z, core):
            send(ref, ref, slot, to_near, "early")
            send(ref, ref, slot, to_across, "fline", inner)

    def early_to_pair(j):
        pieces = early_pieces(held[j], core)
        for (ref, _), slot in zip(pieces, (W_PX, W_PY, W_PD)):
            if j or slot == W_PD:
                send(ref, ref, slot, pair, "early" if j else "early0")

    f_line = line(lambda s: early_pieces(s, core), "fline")
    w_line = line(lambda s: [(wfull.at[dp, s, core], W_Z + s)], "line")
    q_line = line(lambda s: [(q_all.at[2 * s + c], Q_Z + 2 * s + c) for c in range(2)], "qline")

    def send_diag(k):
        dsend[k] = chip_sum(0, k).astype(bf16)
        send(dsend.at[k], rdiag.at[k], G_D + k, xn if k < zh else yn, "sums")

    grad_block(1)
    send_diag(0)
    send_diag(3)
    grad_block(2)
    early_diag()
    send_diag(1)
    send_diag(2)
    q_line[0]()
    q_line[1]()
    send_x(0)
    send_y(3)
    w_line[0]()
    w_line[1]()
    grad_block(3)
    q_line[2]()
    early_own()
    send(cache_keys.at[:, other_cols], kfull.at[pl.ds(keys_one, cached)], K_P, pair, "k")
    send(new_keys.at[:, other_cols], kfull.at[pl.ds(keys_one + cached, fresh)], K_P, pair, "k")
    send(cache_values.at[:, other_cols], vfull.at[pl.ds(keys_one, cached)], V_P, pair, "v")
    send(new_values.at[:, other_cols], vfull.at[pl.ds(keys_one + cached, fresh)], V_P, pair, "v")
    send(frames_hbm, frames.at[1], FRAMES_P, pair, "frames")

    def attention():
        arrived(kfull.at[pl.ds(keys_one, keys_one)], K_P)
        arrived(vfull.at[pl.ds(keys_one, keys_one)], V_P)
        arrived(frames.at[1], FRAMES_P)
        for copy in small_loads:
            copy.wait()
        first_frame = FRAMES_GROUP * group_index[0]
        live_row[...] = jnp.ones_like(live_row)
        for at, which in ((0, 0), (keys_one, 1)):
            f = frames[which]
            ok = (f < first_frame) & (f >= first_frame - WINDOW_FRAMES)
            live_row[:, at : at + cached] = jnp.where(ok, 1.0, 0.0)
        live = live_row[...] > 0.5
        rows_q = 2 * zs * own_q
        lane = lax.broadcasted_iota(jnp.int32, (rows_q, 128), 1)
        stats = jnp.zeros((rows_q, 128), f32)
        for h in range(heads_here):
            cols = slice(h * HEAD, (h + 1) * HEAD)
            q_head = q_all[:, :, cols].reshape(rows_q, HEAD)
            scores = lax.dot_general(
                q_head, kfull[:, cols], (((1,), (1,)), ((), ())), preferred_element_type=f32
            ) * (HEAD ** (-0.5))
            scores = jnp.where(live, scores, -1e30)
            top = jnp.max(scores, axis=1, keepdims=True)
            weights = jnp.where(live, jnp.exp(scores - top), 0.0)
            total = jnp.sum(weights, axis=1, keepdims=True)
            summed = jnp.dot(weights.astype(bf16), vfull[:, cols], preferred_element_type=f32)
            asend[:, :, cols] = summed.astype(bf16).reshape(2 * zs, own_q, HEAD)
            for at, value in ((0, top), (64, total)):
                for part in range(3):
                    piece = value.astype(bf16).astype(f32)
                    stats = jnp.where(lane == at + 16 * part + h, piece, stats)
                    value = value - piece
        asend[:, :, half:] = stats.astype(bf16).reshape(2 * zs, own_q, 128)
        for zt in (near, second, third):
            for ct in (core, other):
                at = zt * 2 + ct
                send(asend.at[at], arecv.at[seq], A_Z, (dp, at), "parts")
        send(asend.at[z * 2 + other], arecv.at[seq], A_Z, pair, "parts")
        arecv[seq] = asend[seq]

    send_y(0)
    send_x(3)
    send_x(1)
    send_y(2)
    w_line[2]()
    arrived(q_all.at[z * 2 + other], Q_Z + z * 2 + other)
    q_line[3]()
    f_line[0]()
    f_line[1]()
    attention()
    send_y(1)
    send_x(2)

    def w_out(j):
        piece = wfull.at[dp, held[j], core, :, late]
        send(piece, piece, W_X + j, xn, "late")
        send(piece, piece, W_Y + j, yn, "late")
        shard_ref = wfull.at[dp, held[j], core]
        send(shard_ref, shard_ref, W_P, pair, "own")

    w_out(1)
    w_line[3]()
    w_out(2)
    w_out(3)
    def grad_in_block(b):
        rows = wfull[order[b]].reshape(block, width)
        step = 512

        def body(t, carry):
            at = pl.ds(pl.multiple_of(t * step, step), step)
            grad_in[at, columns(b)] = lax.dot_general(
                cot[at], rows, (((1,), (1,)), ((), ())), preferred_element_type=f32
            ).astype(bf16)
            return carry

        lax.fori_loop(0, tokens // step, body, 0)

    arrived(wfull.at[dp, :, other], W_P)
    grad_in_block(3)

    def own_sum(k):
        arrived(rx.at[k], G_X + k)
        arrived(ry.at[k], G_Y + k)
        osum[k] = chip_sum(3, k) + rx[k].astype(f32) + ry[k].astype(f32)

    def to_chip(k):
        own_sum(k)

        @pl.when(z != k)
        def _():
            zsend[k] = osum[k].astype(bf16)

        send(zsend.at[k], zrecv.at[z], G_Z, (dp, 2 * k + core), "chip%d" % k, z != k)

    def chain_start():
        @pl.when(outer)
        def _():
            zsend[0] = osum[across].astype(bf16)

        send(zsend.at[0], chain.at[0], C_FAR, to_near, "start", outer)

    def chain_far():
        @pl.when(inner)
        def _():
            arrived(chain.at[0], C_FAR)
            zsend[0] = (osum[far] + chain[0].astype(f32)).astype(bf16)

        send(zsend.at[0], chain.at[1], C_MID, to_across, "far", inner)

    def chain_near():
        @pl.when(inner)
        def _():
            arrived(chain.at[1], C_MID)
            zsend[zs - 1] = (osum[near] + chain[1].astype(f32)).astype(bf16)

        send(zsend.at[zs - 1], chain.at[2], C_END, to_near, "near", inner)

    def from_sides(j):
        cols = late if j else whole
        piece = wfull.at[dp_x, held[j], core, :, cols]
        arrived(piece, W_X + j) if j else None
        if j < zh:
            on = wfull.at[dp_x, held[j], core, :, late]
            send(on, wdiag.at[held[j], core, :, late], W_D, yn, "late")
        send(piece, piece, W_PX, pair, "late" if j else "own")
        piece = wfull.at[dp_y, held[j], core, :, cols]
        arrived(piece, W_Y + j) if j else None
        if j >= zh:
            on = wfull.at[dp_y, held[j], core, :, late]
            send(on, wdiag.at[held[j], core, :, late], W_D, xn, "late")
        send(piece, piece, W_PY, pair, "late" if j else "one")

    def grad_in_sides():
        arrived(wfull.at[dp_x, :, other], W_PX)
        arrived(wfull.at[dp_y, :, other], W_PY)
        rows = jnp.concatenate(
            [wfull[dp_x].reshape(block, width), wfull[dp_y].reshape(block, width)]
        )
        step = 512

        def body(t, carry):
            at = pl.ds(pl.multiple_of(t * step, step), step)
            both = lax.dot_general(
                cot[at], rows, (((1,), (1,)), ((), ())), preferred_element_type=f32
            ).astype(bf16)
            grad_in[at, columns(1)] = both[:, :block]
            grad_in[at, columns(2)] = both[:, block:]
            return carry

        lax.fori_loop(0, tokens // step, body, 0)

    def attention_out():
        arrived(arecv.at[pl.ds(0, 2 * zs - 1)], A_Z)

        def stat(zt, ct, at, h):
            s = arecv[zt * 2 + ct, :, half:].astype(f32)
            return s[:, at + h : at + h + 1] + (
                s[:, at + 16 + h : at + 17 + h] + s[:, at + 32 + h : at + 33 + h]
            )

        for ct in range(2):
            for h in range(heads_here):
                cols = slice(h * HEAD, (h + 1) * HEAD)
                tops = [stat(zt, ct, 0, h) for zt in range(zs)]
                sums = [stat(zt, ct, 64, h) for zt in range(zs)]
                top = functools.reduce(jnp.maximum, tops)
                acc = jnp.zeros((own_q, HEAD), f32)
                total = jnp.zeros((own_q, 1), f32)
                for zt in range(zs):
                    scale = jnp.exp(tops[zt] - top)
                    acc = acc + scale * arecv[zt * 2 + ct, :, cols].astype(f32)
                    total = total + scale * sums[zt]
                mixed[:, ct * half + h * HEAD : ct * half + (h + 1) * HEAD] = (acc / total).astype(bf16)
        gate = jnp.zeros((1, width), f32)
        for s in range(gate_table.shape[0]):
            gate = gate + jnp.where(timestep[0] == s, gate_table[s : s + 1], 0.0)
        projected = jnp.dot(mixed[...], out_weight[...], preferred_element_type=f32)
        stream_out[...] = (stream[...].astype(f32) + gate * projected).astype(bf16)
    def finish_grad():
        factor = float(tokens * parts) ** (-0.5)

        @pl.when(inner)
        def _():
            grad = osum[z]
            arrived(zrecv.at[pl.ds(0, zs - 1)], G_Z)
            for zt in (near, second, third):
                grad = grad + zrecv[zt].astype(f32)
            grad_weight[...] = grad * factor

        @pl.when(outer)
        def _():
            arrived(chain.at[2], C_END)
            grad_weight[...] = (osum[z] + chain[2].astype(f32)) * factor

    own_sum(0)
    own_sum(3)
    chain_start()
    f_line[4]()
    from_sides(0)
    to_chip(1)
    to_chip(2)
    from_sides(1)
    chain_far()
    from_sides(2)
    attention_out()
    from_sides(3)
    chain_near()
    f_line[5]()
    f_line[3]()
    for j in range(zs):
        early_to_pair(j)
    grad_in_sides()
    arrived(wdiag.at[:, core, :, late], W_D)
    for j in range(zs):
        ref = wdiag.at[held[j], core, :, late]
        send(ref, ref, W_PD, pair, "diag")
    finish_grad()
    arrived(wdiag.at[:, other], W_PD)

    all_sent()


def finish_kernel(
    stream_part,
    grad_part,
    weight_part,
    cot,
    wdiag,
    stream_out,
    grad_in,
    grad_weight,
    last,
    sems,
):
    tokens, width = cot.shape
    block = width // 4
    dp = lax.axis_index("dp")
    dp_x = dp + 1 - 2 * lax.rem(dp, 2)
    dp_y = lax.rem(dp + 2, 4)
    dp_d = dp_x + 2 - 4 * (dp_x // 2)
    copies = []

    def put(src, dst):
        copy = pltpu.make_async_copy(src, dst, sems.at[len(copies)])
        copy.start()
        copies.append(copy)

    def columns(b):
        return pl.ds(pl.multiple_of(b * block, 128), block)

    for b in (dp, dp_x, dp_y):
        put(grad_part.at[:, columns(b)], grad_in.at[:, columns(b)])
    put(stream_part, stream_out)
    put(weight_part, grad_weight)
    rows = wdiag[...].reshape(block, width)
    pieces = 4
    step = tokens // pieces
    for t in range(pieces):
        at = slice(t * step, (t + 1) * step)
        last[at] = lax.dot_general(
            cot[at], rows, (((1,), (1,)), ((), ())), preferred_element_type=jnp.float32
        ).astype(last.dtype)
        put(last.at[at], grad_in.at[at, columns(dp_d)])
    for copy in copies:
        copy.wait()


def fused(
    stream,
    queries,
    new_keys,
    new_values,
    cache_keys,
    cache_values,
    cache_frames,
    group_index,
    timestep,
    gate_table,
    attn_out_weight,
    critic_in,
    critic_cot,
    critic_weight,
):
    bf16, f32 = jnp.bfloat16, jnp.float32
    zs = lax.axis_size("seq") // 2
    parts = lax.axis_size(("dp", "seq"))
    tokens, width = critic_in.shape
    own_q = queries.shape[1]
    shard = critic_weight.shape[0]
    cached, fresh = cache_keys.shape[1], new_keys.shape[1]
    half = width // 2
    keys_two = 2 * (cached + fresh)
    vmem, smem = pltpu.VMEM, pltpu.SMEM
    hbm = pl.BlockSpec(memory_space=pltpu.HBM)
    shards = (zs, shard, width)
    parts_out = pl.pallas_call(
        functools.partial(step_kernel, zs, parts),
        out_shape=(
            vmem((own_q, width), bf16),
            vmem((tokens, width), bf16),
            vmem((shard, width), f32),
            vmem((tokens, width), bf16),
            vmem((zs, 2, shard, width), bf16),
        ),
        in_specs=[hbm] * 14,
        out_specs=(pl.BlockSpec(memory_space=vmem),) * 5,
        scratch_shapes=[
            vmem((tokens, width), bf16),
            vmem((width, width), bf16),
            vmem((4, zs, 2, shard, width), bf16),
            vmem((4,) + shards, f32),
            vmem((4,) + shards, bf16),
            vmem((4,) + shards, bf16),
            vmem(shards, bf16),
            vmem(shards, bf16),
            vmem(shards, bf16),
            vmem(shards, bf16),
            vmem(shards, bf16),
            vmem(shards, bf16),
            vmem(shards, f32),
            vmem(shards, bf16),
            vmem(shards, bf16),
            vmem((3, shard, width), bf16),
            vmem((2 * zs, own_q, half), bf16),
            vmem((own_q, half), bf16),
            vmem((keys_two, half), bf16),
            vmem((keys_two, half), bf16),
            vmem((2, 1, cached), jnp.int32),
            vmem((1, keys_two), f32),
            vmem((2 * zs, own_q, half + 128), bf16),
            vmem((2 * zs, own_q, half + 128), bf16),
            vmem((own_q, width), bf16),
            vmem((own_q, width), bf16),
            vmem(gate_table.shape, f32),
            smem((1,), jnp.int32),
            smem((1,), jnp.int32),
            pltpu.SemaphoreType.DMA((22,)),
            pltpu.SemaphoreType.DMA((13 * zs + 14,)),
            pltpu.SemaphoreType.DMA((18,)),
        ],
        compiler_params=pltpu.CompilerParams(
            collective_id=0, has_side_effects=True, vmem_limit_bytes=VMEM_LIMIT
        ),
    )(
        *(
            a if a.shape == (1,) else pltpu.with_memory_space_constraint(a, pltpu.HBM)
            for a in (
                stream[0],
                queries[0],
                new_keys[0],
                new_values[0],
                cache_keys[0],
                cache_values[0],
                cache_frames,
                group_index,
                timestep,
                gate_table,
                attn_out_weight,
                critic_in,
                critic_cot,
                critic_weight,
            )
        )
    )
    stream_out, grad_in, grad_weight = pl.pallas_call(
        finish_kernel,
        out_shape=(
            jax.ShapeDtypeStruct((own_q, width), bf16),
            jax.ShapeDtypeStruct((tokens, width), bf16),
            jax.ShapeDtypeStruct((shard, width), f32),
        ),
        in_specs=[pl.BlockSpec(memory_space=vmem)] * 5,
        out_specs=(hbm,) * 3,
        scratch_shapes=[
            vmem((tokens, width // 4), bf16),
            pltpu.SemaphoreType.DMA((9,)),
        ],
        compiler_params=pltpu.CompilerParams(vmem_limit_bytes=FINISH_LIMIT),
    )(*(pltpu.with_memory_space_constraint(a, vmem) for a in parts_out))
    return (stream_out[None], grad_in, grad_weight)


def local(*args):
    shard, tokens = args[13].shape[0], args[11].shape[0]
    fits = (
        lax.axis_size("dp") == 4
        and lax.axis_size("seq") == 8
        and shard % 16 == 0
        and args[1].shape[1] % 16 == 0
        and args[4].shape[1] % 16 == 0
        and args[1].shape[2] % 512 == 0
        and tokens % 256 == 0
    )
    return fused(*args) if fits else by_collectives(*args)


def solution(mesh):
    return jax.shard_map(
        local,
        mesh=mesh,
        in_specs=(
            P("dp", "seq", None),
            P("dp", "seq", None),
            P("dp", "seq", None),
            P("dp", "seq", None),
            P("dp", "seq", None),
            P("dp", "seq", None),
            P("dp", "seq"),
            P("dp"),
            P("dp"),
            P(),
            P(),
            P(("dp", "seq"), None),
            P(("dp", "seq"), None),
            P(("dp", "seq"), None),
        ),
        out_specs=(P("dp", "seq", None), P(("dp", "seq"), None), P(("dp", "seq"), None)),
        check_vma=False,
    )
```

```python
import functools

import jax
import jax.numpy as jnp
from jax import lax
from jax.experimental import pallas as pl
from jax.experimental.pallas import tpu as pltpu
from jax.sharding import PartitionSpec as P

HEADS = 12
HEAD = 128
FRAMES_GROUP = 3
WINDOW_FRAMES = 9
VMEM_LIMIT = 44 * 1024 * 1024
EARLY = 256
FINISH_LIMIT = 8 * 1024 * 1024


def critic_pass(critic_in, critic_cot, critic_weight):
    grad_in = lax.dot_general(
        critic_cot,
        lax.all_gather(critic_weight, ("dp", "seq"), axis=0, tiled=True),
        (((1,), (1,)), ((), ())),
        preferred_element_type=jnp.float32,
    ).astype(jnp.bfloat16)
    factor = float(critic_in.shape[0] * lax.axis_size(("dp", "seq"))) ** (-0.5)
    whole_term = (
        lax.dot_general(
            critic_in, critic_cot, (((0,), (0,)), ((), ())), preferred_element_type=jnp.float32
        )
        * factor
    )
    grad_weight = lax.psum_scatter(whole_term, ("dp", "seq"), scatter_dimension=0, tiled=True)
    return (grad_in, grad_weight)


def by_collectives(
    stream,
    queries,
    new_keys,
    new_values,
    cache_keys,
    cache_values,
    cache_frames,
    group_index,
    timestep,
    gate_table,
    attn_out_weight,
    critic_in,
    critic_cot,
    critic_weight,
):
    query_local = queries[0]
    own_rows = query_local.shape[0]
    width = query_local.shape[1]
    scale = HEAD ** (-0.5)
    first_frame = FRAMES_GROUP * group_index[0]
    frames = cache_frames[0]
    live_cache = (frames < first_frame) & (frames >= first_frame - WINDOW_FRAMES)
    live_local = jnp.concatenate([live_cache, jnp.ones((own_rows,), dtype=bool)])
    keys_local = jnp.concatenate([cache_keys[0], new_keys[0]], axis=0)
    values_local = jnp.concatenate([cache_values[0], new_values[0]], axis=0)
    all_queries = lax.all_gather(queries, "seq", axis=1, tiled=True)[0]
    total_rows = all_queries.shape[0]
    query_heads = all_queries.reshape(total_rows, HEADS, HEAD)
    key_heads = keys_local.reshape(-1, HEADS, HEAD)
    value_heads = values_local.reshape(-1, HEADS, HEAD)
    scores = (
        jnp.einsum("qhd,khd->hqk", query_heads, key_heads, preferred_element_type=jnp.float32)
        * scale
    )
    scores = jnp.where(live_local[None, None, :], scores, -1e30)
    local_top = jnp.max(scores, axis=2)
    global_top = lax.pmax(local_top, "seq")
    weights = jnp.where(live_local[None, None, :], jnp.exp(scores - global_top[:, :, None]), 0.0)
    totals = jnp.sum(weights, axis=2)
    summed = jnp.einsum(
        "hqk,khd->qhd",
        weights.astype(jnp.bfloat16),
        value_heads,
        preferred_element_type=jnp.float32,
    )
    own_sums, own_totals = (
        lax.psum_scatter(summed.reshape(total_rows, width), "seq", scatter_dimension=0, tiled=True),
        lax.psum_scatter(totals.T, "seq", scatter_dimension=0, tiled=True),
    )
    mixed = (
        (own_sums.reshape(own_rows, HEADS, HEAD) / own_totals[:, :, None])
        .reshape(own_rows, width)
        .astype(jnp.bfloat16)
    )
    projected = jnp.dot(mixed, attn_out_weight, preferred_element_type=jnp.float32)
    onehot = (
        timestep[:, None] == jnp.arange(gate_table.shape[0], dtype=jnp.int32)[None, :]
    ).astype(jnp.float32)
    gate = jnp.dot(onehot, gate_table, precision=lax.Precision.HIGHEST)
    stream_out = (stream[0].astype(jnp.float32) + gate * projected).astype(jnp.bfloat16)[None]
    grad_in, grad_weight = critic_pass(critic_in, critic_cot, critic_weight)
    return (stream_out, grad_in, grad_weight)


def step_kernel(
    zs,
    parts,
    stream_hbm,
    queries,
    new_keys,
    new_values,
    cache_keys,
    cache_values,
    frames_hbm,
    group_hbm,
    timestep_hbm,
    gate_hbm,
    out_weight_hbm,
    critic_in,
    critic_cot,
    weight_hbm,
    stream_out,
    grad_in,
    grad_weight,
    cot,
    wdiag,
    cin,
    out_weight,
    wfull,
    gmine,
    psend,
    precv,
    dsend,
    xsend,
    ysend,
    rdiag,
    rx,
    ry,
    osum,
    zsend,
    zrecv,
    chain,
    q_all,
    q_other,
    kfull,
    vfull,
    frames,
    live_row,
    asend,
    arecv,
    mixed,
    stream,
    gate_table,
    group_index,
    timestep,
    send_sems,
    recv_sems,
    local_sems,
):
    f32, bf16 = jnp.float32, jnp.bfloat16
    dp, seq = lax.axis_index("dp"), lax.axis_index("seq")
    z, core = seq // 2, lax.rem(seq, 2)
    other = 1 - core
    tokens, width = cin.shape
    block = width // 4
    half = width // 2
    whole, early = pl.ds(0, width), pl.ds(width - EARLY, EARLY)
    late = pl.ds(0, width - EARLY)
    own_q = queries.shape[0]
    cached, fresh = cache_keys.shape[0], new_keys.shape[0]
    keys_one = cached + fresh
    heads_here = half // HEAD
    zh = zs // 2
    dp_x = dp + 1 - 2 * lax.rem(dp, 2)
    dp_y = lax.rem(dp + 2, 4)
    dp_d = dp_x + 2 - 4 * (dp_x // 2)
    order = (dp_d, dp_x, dp_y, dp)
    xn, yn, pair = (dp_x, seq), (dp_y, seq), (dp, z * 2 + other)

    near = z + 1 - 2 * lax.rem(z, 2)
    across = zs - 1 - z
    far = zs - 1 - near
    inner = (z == 1) | (z == 2)
    outer = jnp.logical_not(inner)
    to_near, to_across = (dp, near * 2 + core), (dp, across * 2 + core)
    second = jnp.where(inner, across, far)
    third = jnp.where(inner, far, across)
    held = (z, near, second, third)

    other_cols = pl.ds(pl.multiple_of(other * half, 128), half)
    own_cols = pl.ds(pl.multiple_of(core * half, 128), half)

    started = []

    def load(src, dst):
        copy = pltpu.make_async_copy(src, dst, local_sems.at[len(started)])
        copy.start()
        started.append(copy)
        return copy

    def columns(b):
        return pl.ds(pl.multiple_of(order[b] * block, 128), block)

    weight_load = load(weight_hbm, wfull.at[dp, z, core])
    q_load = load(queries.at[:, own_cols], q_all.at[seq])
    q_other_load = load(queries.at[:, other_cols], q_other)
    cot_load = load(critic_cot, cot)
    cin_loads = [load(critic_in.at[:, columns(b)], cin.at[:, columns(b)]) for b in range(4)]
    small_loads = [
        load(cache_keys.at[:, own_cols], kfull.at[pl.ds(0, cached)]),
        load(new_keys.at[:, own_cols], kfull.at[pl.ds(cached, fresh)]),
        load(cache_values.at[:, own_cols], vfull.at[pl.ds(0, cached)]),
        load(new_values.at[:, own_cols], vfull.at[pl.ds(cached, fresh)]),
        load(frames_hbm, frames.at[0]),
        load(group_hbm, group_index),
        load(timestep_hbm, timestep),
        load(gate_hbm, gate_table),
        load(stream_hbm, stream),
        load(out_weight_hbm, out_weight),
    ]

    barrier = pltpu.get_barrier_semaphore()
    def greet(peer):
        pl.semaphore_signal(
            barrier, inc=1, device_id=peer, device_id_type=pl.DeviceIdType.MESH
        )

    peers = [xn, yn, pair, to_near, (dp, near * 2 + other)]
    for peer in peers:
        greet(peer)

    @pl.when(inner)
    def _():
        greet(to_across)
        greet((dp, across * 2 + other))

    pl.semaphore_wait(barrier, len(peers) + 2 * inner.astype(jnp.int32))

    groups = {}

    def remote(src, dst, slot, peer, n):
        return pltpu.make_async_remote_copy(
            src_ref=src,
            dst_ref=dst,
            send_sem=send_sems.at[n],
            recv_sem=recv_sems.at[slot],
            device_id=peer,
            device_id_type=pl.DeviceIdType.MESH,
        )

    def send(src, dst, slot, peer, group, when=None):
        n = groups.setdefault(group, len(groups))
        copy = remote(src, dst, slot, peer, n)
        if when is None:
            copy.start()
        else:
            pl.when(when)(copy.start)

    def all_sent():
        eight = precv.at[pl.ds(0, 2)]
        twelve = precv.at[pl.ds(0, 3)]
        three = pl.ds(0, 3)
        totals = {
            "own": (eight, None),
            "one": (precv.at[0, 0], None),
            "line": (precv.at[0], inner),
            "psend": (precv, None),
            "sums": (twelve, None),
            "late": (precv.at[:, :, :, late], None),
            "diag": (precv.at[0, :, :, late], None),
            "chip1": (precv.at[0, 0], z != 1),
            "chip2": (precv.at[0, 0], z != 2),
            "start": (precv.at[0, 0], outer),
            "far": (precv.at[0, 0], inner),
            "near": (precv.at[0, 0], inner),
            "early": (precv.at[three, :, :, early], None),
            "early0": (precv.at[0, 0, :, early], None),
            "earlyd": (precv.at[0, 0, :, early], None),
            "fline": (precv.at[three, :, :, early], inner),
            "q": (q_all.at[three], None),
            "qline": (q_all, inner),
            "k": (kfull.at[pl.ds(0, keys_one)], None),
            "v": (vfull.at[pl.ds(0, keys_one)], None),
            "frames": (frames.at[0], None),
            "parts": (arecv.at[pl.ds(0, 2 * zs - 1)], None),
        }
        for group, n in groups.items():
            view, when = totals[group]
            wait = remote(view, view, 0, pair, n).wait_send
            if when is None:
                wait()
            else:
                pl.when(when)(wait)

    def arrived(dst, slot):
        remote(dst, dst, slot, pair, 0).wait_recv()

    W_Z, W_X, W_Y, F_Z, Q_Z = 0, zs, 2 * zs, 3 * zs, 4 * zs
    G_P, G_D, G_X, G_Y = 6 * zs, 10 * zs, 11 * zs, 12 * zs
    W_P, W_PX, W_PY, W_PD, W_D, F_OWN = (13 * zs + i for i in range(6))
    K_P, V_P, FRAMES_P, A_Z, G_Z = (13 * zs + 6 + i for i in range(5))
    C_FAR, C_MID, C_END = (13 * zs + 11 + i for i in range(3))

    q_load.wait()
    q_other_load.wait()
    for chip, when in ((near, None), (across, inner)):
        send(q_all.at[seq], q_all.at[seq], Q_Z + seq, (dp, chip * 2 + core), "qline" if when is not None else "q", when)
        send(q_other, q_all.at[seq], Q_Z + seq, (dp, chip * 2 + other), "qline" if when is not None else "q", when)
    send(q_other, q_all.at[seq], Q_Z + seq, pair, "q")
    mine = wfull.at[dp, z, core]
    weight_load.wait()
    send(mine, mine, W_Z + z, to_near, "own")
    send(mine, mine, W_Z + z, to_across, "line", inner)
    send(mine, mine, W_X, xn, "own")
    send(mine, mine, W_Y, yn, "own")
    send(mine, mine, W_P, pair, "own")

    def grad_block(b):
        cin_loads[b].wait()
        acc = lax.dot_general(
            cin[:, columns(b)],
            cot[...],
            (((0,), (0,)), ((), ())),
            preferred_element_type=f32,
        )
        shard = block // (2 * zs)
        for k in range(zs):
            lo = acc[2 * k * shard : (2 * k + 1) * shard]
            hi = acc[(2 * k + 1) * shard : (2 * k + 2) * shard]
            gmine[b, k] = jnp.where(core == 0, lo, hi)
            psend[b, k] = jnp.where(core == 0, hi, lo).astype(bf16)
        for k in range(zs):
            send(psend.at[b, k], precv.at[b, k], G_P + b * zs + k, pair, "psend")

    def chip_sum(b, k):
        arrived(precv.at[b, k], G_P + b * zs + k)
        return gmine[b, k] + precv[b, k].astype(f32)

    cot_load.wait()
    grad_block(0)

    def send_x(k):
        total = chip_sum(1, k)
        if k >= zh:
            arrived(rdiag.at[k], G_D + k)
            total = total + rdiag[k].astype(f32)
        xsend[k] = total.astype(bf16)
        send(xsend.at[k], rx.at[k], G_X + k, xn, "sums")

    def send_y(k):
        total = chip_sum(2, k)
        if k < zh:
            arrived(rdiag.at[k], G_D + k)
            total = total + rdiag[k].astype(f32)
        ysend[k] = total.astype(bf16)
        send(ysend.at[k], ry.at[k], G_Y + k, yn, "sums")

    def line(of, group):
        def take(source):
            if group == "fline":
                arrived(precv.at[0, pl.ds(0, 3), :, early], F_Z + source)
                return
            for ref, slot in of(source):
                arrived(ref, slot)

        def pass_on(source, peer):
            for ref, slot in of(source):
                send(ref, ref, slot, peer, group, inner)

        def first():
            take(near)
            pass_on(near, to_across)

        def inner_second():
            pl.when(inner)(lambda: take(across))
            pass_on(across, to_near)

        def both_third():
            take(far)
            pass_on(far, to_near)

        def outer_last():
            pl.when(outer)(lambda: take(across))

        def inner_third():
            pl.when(inner)(lambda: take(far))
            pass_on(far, to_near)

        def outer_third():
            pl.when(outer)(lambda: take(far))

        return first, inner_second, both_third, outer_last, inner_third, outer_third

    def early_pieces(s, c):
        return [
            (wfull.at[dp_x, s, c, :, early], F_Z + s),
            (wfull.at[dp_y, s, c, :, early], F_Z + s),
            (wdiag.at[s, c, :, early], F_Z + s),
        ]

    def early_diag():
        arrived(wfull.at[dp_x, z, core], W_X)
        arrived(wfull.at[dp_y, z, core], W_Y)
        for way, peer, when in ((dp_x, yn, core == 0), (dp_y, xn, core == 1)):
            send(
                wfull.at[way, z, core, :, early], wdiag.at[z, core, :, early], F_OWN, peer, "earlyd", when
            )

    def early_own():
        arrived(wdiag.at[z, core, :, early], F_OWN)
        for ref, slot in early_pieces(z, core):
            send(ref, ref, slot, to_near, "early")
            send(ref, ref, slot, to_across, "fline", inner)

    def early_to_pair(j):
        pieces = early_pieces(held[j], core)
        for (ref, _), slot in zip(pieces, (W_PX, W_PY, W_PD)):
            if j or slot == W_PD:
                send(ref, ref, slot, pair, "early" if j else "early0")

    f_line = line(lambda s: early_pieces(s, core), "fline")
    w_line = line(lambda s: [(wfull.at[dp, s, core], W_Z + s)], "line")
    q_line = line(lambda s: [(q_all.at[2 * s + c], Q_Z + 2 * s + c) for c in range(2)], "qline")

    def send_diag(k):
        dsend[k] = chip_sum(0, k).astype(bf16)
        send(dsend.at[k], rdiag.at[k], G_D + k, xn if k < zh else yn, "sums")

    grad_block(1)
    send_diag(0)
    send_diag(3)
    grad_block(2)
    early_diag()
    send_diag(1)
    send_diag(2)
    q_line[0]()
    q_line[1]()
    send_x(0)
    send_y(3)
    w_line[0]()
    w_line[1]()
    grad_block(3)
    q_line[2]()
    early_own()
    send(cache_keys.at[:, other_cols], kfull.at[pl.ds(keys_one, cached)], K_P, pair, "k")
    send(new_keys.at[:, other_cols], kfull.at[pl.ds(keys_one + cached, fresh)], K_P, pair, "k")
    send(cache_values.at[:, other_cols], vfull.at[pl.ds(keys_one, cached)], V_P, pair, "v")
    send(new_values.at[:, other_cols], vfull.at[pl.ds(keys_one + cached, fresh)], V_P, pair, "v")
    send(frames_hbm, frames.at[1], FRAMES_P, pair, "frames")

    def attention():
        arrived(kfull.at[pl.ds(keys_one, keys_one)], K_P)
        arrived(vfull.at[pl.ds(keys_one, keys_one)], V_P)
        arrived(frames.at[1], FRAMES_P)
        for copy in small_loads:
            copy.wait()
        first_frame = FRAMES_GROUP * group_index[0]
        live_row[...] = jnp.ones_like(live_row)
        for at, which in ((0, 0), (keys_one, 1)):
            f = frames[which]
            ok = (f < first_frame) & (f >= first_frame - WINDOW_FRAMES)
            live_row[:, at : at + cached] = jnp.where(ok, 1.0, 0.0)
        live = live_row[...] > 0.5
        rows_q = 2 * zs * own_q
        lane = lax.broadcasted_iota(jnp.int32, (rows_q, 128), 1)
        stats = jnp.zeros((rows_q, 128), f32)
        for h in range(heads_here):
            cols = slice(h * HEAD, (h + 1) * HEAD)
            q_head = q_all[:, :, cols].reshape(rows_q, HEAD)
            scores = lax.dot_general(
                q_head, kfull[:, cols], (((1,), (1,)), ((), ())), preferred_element_type=f32
            ) * (HEAD ** (-0.5))
            scores = jnp.where(live, scores, -1e30)
            top = jnp.max(scores, axis=1, keepdims=True)
            weights = jnp.where(live, jnp.exp(scores - top), 0.0)
            total = jnp.sum(weights, axis=1, keepdims=True)
            summed = jnp.dot(weights.astype(bf16), vfull[:, cols], preferred_element_type=f32)
            asend[:, :, cols] = summed.astype(bf16).reshape(2 * zs, own_q, HEAD)
            for at, value in ((0, top), (64, total)):
                for part in range(3):
                    piece = value.astype(bf16).astype(f32)
                    stats = jnp.where(lane == at + 16 * part + h, piece, stats)
                    value = value - piece
        asend[:, :, half:] = stats.astype(bf16).reshape(2 * zs, own_q, 128)
        for zt in (near, second, third):
            for ct in (core, other):
                at = zt * 2 + ct
                send(asend.at[at], arecv.at[seq], A_Z, (dp, at), "parts")
        send(asend.at[z * 2 + other], arecv.at[seq], A_Z, pair, "parts")
        arecv[seq] = asend[seq]

    send_y(0)
    send_x(3)
    send_x(1)
    send_y(2)
    w_line[2]()
    arrived(q_all.at[z * 2 + other], Q_Z + z * 2 + other)
    q_line[3]()
    f_line[0]()
    f_line[1]()
    attention()
    send_y(1)
    send_x(2)

    def w_out(j):
        piece = wfull.at[dp, held[j], core, :, late]
        send(piece, piece, W_X + j, xn, "late")
        send(piece, piece, W_Y + j, yn, "late")
        shard_ref = wfull.at[dp, held[j], core]
        send(shard_ref, shard_ref, W_P, pair, "own")

    w_out(1)
    w_line[3]()
    w_out(2)
    w_out(3)
    def grad_in_block(b):
        rows = wfull[order[b]].reshape(block, width)
        step = 512

        def body(t, carry):
            at = pl.ds(pl.multiple_of(t * step, step), step)
            grad_in[at, columns(b)] = lax.dot_general(
                cot[at], rows, (((1,), (1,)), ((), ())), preferred_element_type=f32
            ).astype(bf16)
            return carry

        lax.fori_loop(0, tokens // step, body, 0)

    arrived(wfull.at[dp, :, other], W_P)
    grad_in_block(3)

    def own_sum(k):
        arrived(rx.at[k], G_X + k)
        arrived(ry.at[k], G_Y + k)
        osum[k] = chip_sum(3, k) + rx[k].astype(f32) + ry[k].astype(f32)

    def to_chip(k):
        own_sum(k)

        @pl.when(z != k)
        def _():
            zsend[k] = osum[k].astype(bf16)

        send(zsend.at[k], zrecv.at[z], G_Z, (dp, 2 * k + core), "chip%d" % k, z != k)

    def chain_start():
        @pl.when(outer)
        def _():
            zsend[0] = osum[across].astype(bf16)

        send(zsend.at[0], chain.at[0], C_FAR, to_near, "start", outer)

    def chain_far():
        @pl.when(inner)
        def _():
            arrived(chain.at[0], C_FAR)
            zsend[0] = (osum[far] + chain[0].astype(f32)).astype(bf16)

        send(zsend.at[0], chain.at[1], C_MID, to_across, "far", inner)

    def chain_near():
        @pl.when(inner)
        def _():
            arrived(chain.at[1], C_MID)
            zsend[zs - 1] = (osum[near] + chain[1].astype(f32)).astype(bf16)

        send(zsend.at[zs - 1], chain.at[2], C_END, to_near, "near", inner)

    def from_sides(j):
        cols = late if j else whole
        piece = wfull.at[dp_x, held[j], core, :, cols]
        arrived(piece, W_X + j) if j else None
        if j < zh:
            on = wfull.at[dp_x, held[j], core, :, late]
            send(on, wdiag.at[held[j], core, :, late], W_D, yn, "late")
        send(piece, piece, W_PX, pair, "late" if j else "own")
        piece = wfull.at[dp_y, held[j], core, :, cols]
        arrived(piece, W_Y + j) if j else None
        if j >= zh:
            on = wfull.at[dp_y, held[j], core, :, late]
            send(on, wdiag.at[held[j], core, :, late], W_D, xn, "late")
        send(piece, piece, W_PY, pair, "late" if j else "one")

    def grad_in_sides():
        arrived(wfull.at[dp_x, :, other], W_PX)
        arrived(wfull.at[dp_y, :, other], W_PY)
        rows = jnp.concatenate(
            [wfull[dp_x].reshape(block, width), wfull[dp_y].reshape(block, width)]
        )
        step = 512

        def body(t, carry):
            at = pl.ds(pl.multiple_of(t * step, step), step)
            both = lax.dot_general(
                cot[at], rows, (((1,), (1,)), ((), ())), preferred_element_type=f32
            ).astype(bf16)
            grad_in[at, columns(1)] = both[:, :block]
            grad_in[at, columns(2)] = both[:, block:]
            return carry

        lax.fori_loop(0, tokens // step, body, 0)

    def attention_out():
        arrived(arecv.at[pl.ds(0, 2 * zs - 1)], A_Z)

        def stat(zt, ct, at, h):
            s = arecv[zt * 2 + ct, :, half:].astype(f32)
            return s[:, at + h : at + h + 1] + (
                s[:, at + 16 + h : at + 17 + h] + s[:, at + 32 + h : at + 33 + h]
            )

        for ct in range(2):
            for h in range(heads_here):
                cols = slice(h * HEAD, (h + 1) * HEAD)
                tops = [stat(zt, ct, 0, h) for zt in range(zs)]
                sums = [stat(zt, ct, 64, h) for zt in range(zs)]
                top = functools.reduce(jnp.maximum, tops)
                acc = jnp.zeros((own_q, HEAD), f32)
                total = jnp.zeros((own_q, 1), f32)
                for zt in range(zs):
                    scale = jnp.exp(tops[zt] - top)
                    acc = acc + scale * arecv[zt * 2 + ct, :, cols].astype(f32)
                    total = total + scale * sums[zt]
                mixed[:, ct * half + h * HEAD : ct * half + (h + 1) * HEAD] = (acc / total).astype(bf16)
        gate = jnp.zeros((1, width), f32)
        for s in range(gate_table.shape[0]):
            gate = gate + jnp.where(timestep[0] == s, gate_table[s : s + 1], 0.0)
        projected = jnp.dot(mixed[...], out_weight[...], preferred_element_type=f32)
        stream_out[...] = (stream[...].astype(f32) + gate * projected).astype(bf16)
    def finish_grad():
        factor = float(tokens * parts) ** (-0.5)

        @pl.when(inner)
        def _():
            grad = osum[z]
            arrived(zrecv.at[pl.ds(0, zs - 1)], G_Z)
            for zt in (near, second, third):
                grad = grad + zrecv[zt].astype(f32)
            grad_weight[...] = grad * factor

        @pl.when(outer)
        def _():
            arrived(chain.at[2], C_END)
            grad_weight[...] = (osum[z] + chain[2].astype(f32)) * factor

    own_sum(0)
    own_sum(3)
    chain_start()
    f_line[4]()
    from_sides(0)
    to_chip(1)
    to_chip(2)
    from_sides(1)
    chain_far()
    from_sides(2)
    attention_out()
    from_sides(3)
    chain_near()
    f_line[5]()
    f_line[3]()
    for j in range(zs):
        early_to_pair(j)
    grad_in_sides()
    arrived(wdiag.at[:, core, :, late], W_D)
    for j in range(zs):
        ref = wdiag.at[held[j], core, :, late]
        send(ref, ref, W_PD, pair, "diag")
    finish_grad()
    arrived(wdiag.at[:, other], W_PD)

    all_sent()


def finish_kernel(
    stream_part,
    grad_part,
    weight_part,
    cot,
    wdiag,
    stream_out,
    grad_in,
    grad_weight,
    last,
    sems,
):
    tokens, width = cot.shape
    block = width // 4
    dp = lax.axis_index("dp")
    dp_x = dp + 1 - 2 * lax.rem(dp, 2)
    dp_y = lax.rem(dp + 2, 4)
    dp_d = dp_x + 2 - 4 * (dp_x // 2)
    copies = []

    def put(src, dst):
        copy = pltpu.make_async_copy(src, dst, sems.at[len(copies)])
        copy.start()
        copies.append(copy)

    def columns(b):
        return pl.ds(pl.multiple_of(b * block, 128), block)

    for b in (dp, dp_x, dp_y):
        put(grad_part.at[:, columns(b)], grad_in.at[:, columns(b)])
    put(stream_part, stream_out)
    put(weight_part, grad_weight)
    rows = wdiag[...].reshape(block, width)
    pieces = 4
    step = tokens // pieces
    for t in range(pieces):
        at = slice(t * step, (t + 1) * step)
        last[at] = lax.dot_general(
            cot[at], rows, (((1,), (1,)), ((), ())), preferred_element_type=jnp.float32
        ).astype(last.dtype)
        put(last.at[at], grad_in.at[at, columns(dp_d)])
    for copy in copies:
        copy.wait()


def fused(
    stream,
    queries,
    new_keys,
    new_values,
    cache_keys,
    cache_values,
    cache_frames,
    group_index,
    timestep,
    gate_table,
    attn_out_weight,
    critic_in,
    critic_cot,
    critic_weight,
):
    bf16, f32 = jnp.bfloat16, jnp.float32
    zs = lax.axis_size("seq") // 2
    parts = lax.axis_size(("dp", "seq"))
    tokens, width = critic_in.shape
    own_q = queries.shape[1]
    shard = critic_weight.shape[0]
    cached, fresh = cache_keys.shape[1], new_keys.shape[1]
    half = width // 2
    keys_two = 2 * (cached + fresh)
    vmem, smem = pltpu.VMEM, pltpu.SMEM
    hbm = pl.BlockSpec(memory_space=pltpu.HBM)
    shards = (zs, shard, width)
    parts_out = pl.pallas_call(
        functools.partial(step_kernel, zs, parts),
        out_shape=(
            vmem((own_q, width), bf16),
            vmem((tokens, width), bf16),
            vmem((shard, width), f32),
            vmem((tokens, width), bf16),
            vmem((zs, 2, shard, width), bf16),
        ),
        in_specs=[hbm] * 14,
        out_specs=(pl.BlockSpec(memory_space=vmem),) * 5,
        scratch_shapes=[
            vmem((tokens, width), bf16),
            vmem((width, width), bf16),
            vmem((4, zs, 2, shard, width), bf16),
            vmem((4,) + shards, f32),
            vmem((4,) + shards, bf16),
            vmem((4,) + shards, bf16),
            vmem(shards, bf16),
            vmem(shards, bf16),
            vmem(shards, bf16),
            vmem(shards, bf16),
            vmem(shards, bf16),
            vmem(shards, bf16),
            vmem(shards, f32),
            vmem(shards, bf16),
            vmem(shards, bf16),
            vmem((3, shard, width), bf16),
            vmem((2 * zs, own_q, half), bf16),
            vmem((own_q, half), bf16),
            vmem((keys_two, half), bf16),
            vmem((keys_two, half), bf16),
            vmem((2, 1, cached), jnp.int32),
            vmem((1, keys_two), f32),
            vmem((2 * zs, own_q, half + 128), bf16),
            vmem((2 * zs, own_q, half + 128), bf16),
            vmem((own_q, width), bf16),
            vmem((own_q, width), bf16),
            vmem(gate_table.shape, f32),
            smem((1,), jnp.int32),
            smem((1,), jnp.int32),
            pltpu.SemaphoreType.DMA((22,)),
            pltpu.SemaphoreType.DMA((13 * zs + 14,)),
            pltpu.SemaphoreType.DMA((18,)),
        ],
        compiler_params=pltpu.CompilerParams(
            collective_id=0, has_side_effects=True, vmem_limit_bytes=VMEM_LIMIT
        ),
    )(
        *(
            a if a.shape == (1,) else pltpu.with_memory_space_constraint(a, pltpu.HBM)
            for a in (
                stream[0],
                queries[0],
                new_keys[0],
                new_values[0],
                cache_keys[0],
                cache_values[0],
                cache_frames,
                group_index,
                timestep,
                gate_table,
                attn_out_weight,
                critic_in,
                critic_cot,
                critic_weight,
            )
        )
    )
    stream_out, grad_in, grad_weight = pl.pallas_call(
        finish_kernel,
        out_shape=(
            jax.ShapeDtypeStruct((own_q, width), bf16),
            jax.ShapeDtypeStruct((tokens, width), bf16),
            jax.ShapeDtypeStruct((shard, width), f32),
        ),
        in_specs=[pl.BlockSpec(memory_space=vmem)] * 5,
        out_specs=(hbm,) * 3,
        scratch_shapes=[
            vmem((tokens, width // 4), bf16),
            pltpu.SemaphoreType.DMA((9,)),
        ],
        compiler_params=pltpu.CompilerParams(vmem_limit_bytes=FINISH_LIMIT),
    )(*(pltpu.with_memory_space_constraint(a, vmem) for a in parts_out))
    return (stream_out[None], grad_in, grad_weight)


def local(*args):
    shard, tokens = args[13].shape[0], args[11].shape[0]
    fits = (
        lax.axis_size("dp") == 4
        and lax.axis_size("seq") == 8
        and shard % 16 == 0
        and args[1].shape[1] % 16 == 0
        and args[4].shape[1] % 16 == 0
        and args[1].shape[2] % 512 == 0
        and tokens % 256 == 0
    )
    return fused(*args) if fits else by_collectives(*args)


def solution(mesh):
    return jax.shard_map(
        local,
        mesh=mesh,
        in_specs=(
            P("dp", "seq", None),
            P("dp", "seq", None),
            P("dp", "seq", None),
            P("dp", "seq", None),
            P("dp", "seq", None),
            P("dp", "seq", None),
            P("dp", "seq"),
            P("dp"),
            P("dp"),
            P(),
            P(),
            P(("dp", "seq"), None),
            P(("dp", "seq"), None),
            P(("dp", "seq"), None),
        ),
        out_specs=(P("dp", "seq", None), P(("dp", "seq"), None), P(("dp", "seq"), None)),
        check_vma=False,
    )
```
